32 devices in a mesh: seq: 8 (over z, y), dp: 4 (over x, core).
Axes of the slice: x: 2, y: 2, z: 4, core: 2. Of those that a mesh axis runs over, the one named last changes fastest.
Arguments:
- attention_queries: bfloat16 [8, 2, 256, 4096], P('seq', None, 'dp'), parts along dimension 2, may hold values from -5.5 to 5.5
- attention_keys: bfloat16 [8, 2, 256, 512], P('seq', None, 'dp'), parts along dimension 2, may hold values from -7.5 to 7.5
- attention_values: bfloat16 [8, 2, 256, 512], P('seq', None, 'dp'), parts along dimension 2, may hold values from -6 to 6
- attention_output: bfloat16 [8, 2, 256, 4096], P('seq', None, 'dp'), parts along dimension 2, may hold values from -6 to 6
- output_gradient: bfloat16 [8, 2, 256, 4096], P('seq', None, 'dp'), parts along dimension 2, may hold values from -48 to 48
- logsumexp_rows: float32 [8, 2, 256, 32], P('seq', None, 'dp'), parts along dimension 2, as said below
Outputs:
- grad_query: float32 [8, 2, 256, 4096], P('seq', None, 'dp'), parts along dimension 2
- key_gradient: float32 [8, 2, 256, 512], P('seq', None, 'dp'), parts along dimension 2
- value_gradient: float32 [8, 2, 256, 512], P('seq', None, 'dp'), parts along dimension 2
The draws below stay inside these ranges and needn't reach their ends.
There are 4 independent parts, one for each index of `dp`. The reference program is written for one: setup_inputs(seed, part) draws one part's arguments, and reference() takes and returns one part's arrays. A program takes and returns all parts, laid end to end along the dimension named above; each array names one. Nothing has to cross between parts.
Inputs may be any that keep to these rules, and one draw needn't show every extreme that they name: logsumexp_rows[i, h] is the logarithm of the sum over key positions t <= i of exp(scores[h, i, t]), computed from attention_queries and attention_keys in float32.
All inputs are finite; a program needn't handle non-finite values.
Results may differ from the reference program's by a relative error of at most 0.0003.
Values may be sent and summed in bfloat16 or wider, within the bound.
A program may use at most 128 MiB of HBM per device.

```python
import jax
import jax.numpy as jnp
from jax import lax

HQ = 32
KEY_VALUE_HEADS = 4
HEAD_SIZE = 128
QUERY_PER_KV = 8
BLOCK_TOKENS = 64
BLOCK_PAIRS = 8


def draw_attention_queries(key, part):
    complete_shape = (BLOCK_PAIRS, 2, BLOCK_TOKENS, HQ * HEAD_SIZE)
    sampled_inputs = jnp.clip(jax.random.normal(jax.random.fold_in(key, 11), complete_shape, jnp.float32), -4.0, 4.0)
    return sampled_inputs.astype(jnp.bfloat16)


def draw_attention_keys(key, part):
    complete_shape = (BLOCK_PAIRS, 2, BLOCK_TOKENS, KEY_VALUE_HEADS, HEAD_SIZE)
    sampled_inputs = jnp.clip(jax.random.normal(jax.random.fold_in(key, 13), complete_shape, jnp.float32), -4.0, 4.0)
    sampled_inputs = sampled_inputs.reshape(BLOCK_PAIRS, 2, BLOCK_TOKENS, KEY_VALUE_HEADS * HEAD_SIZE)
    return sampled_inputs.astype(jnp.bfloat16)


def sequence_row_list(blocks):
    width = blocks.shape[-1]
    earlier_half = blocks[:, 0].reshape(BLOCK_PAIRS * BLOCK_TOKENS, width)
    later_half = blocks[::-1, 1].reshape(BLOCK_PAIRS * BLOCK_TOKENS, width)
    return jnp.concatenate([earlier_half, later_half], axis=0)


def draw_logsumexp_rows(key, part):
    sequence_length = 2 * BLOCK_PAIRS * BLOCK_TOKENS
    span_rows = 2 * BLOCK_TOKENS
    query_values_list = sequence_row_list(draw_attention_queries(key, part).astype(jnp.float32)).reshape(sequence_length, KEY_VALUE_HEADS, QUERY_PER_KV, HEAD_SIZE)
    every_key = sequence_row_list(draw_attention_keys(key, part).astype(jnp.float32)).reshape(sequence_length, KEY_VALUE_HEADS, HEAD_SIZE)
    key_pos = jnp.arange(sequence_length, dtype=jnp.int32)

    def per_block(block_index):
        first_row = (block_index * span_rows).astype(jnp.int32)
        query_blk = lax.dynamic_slice_in_dim(query_values_list, first_row, span_rows, 0)
        query_pos = first_row + jnp.arange(span_rows, dtype=jnp.int32)
        allowed = key_pos[None, :] <= query_pos[:, None]
        scores = HEAD_SIZE ** (-0.5) * jnp.einsum('qhgd,khd->hgqk', query_blk, every_key, precision=lax.Precision.HIGHEST)
        largest = jnp.max(jnp.where(allowed, scores, -1e+30), axis=-1, keepdims=True)
        expsum = jnp.sum(jnp.where(allowed, jnp.exp(scores - largest), 0.0), axis=-1, keepdims=True)
        totals = (largest + jnp.log(expsum))[..., 0]
        return totals.transpose(2, 0, 1).reshape(span_rows, HQ)
    rows_all = lax.map(per_block, jnp.arange(BLOCK_PAIRS, dtype=jnp.int32)).reshape(sequence_length, HQ)
    earlier_half = rows_all[:BLOCK_PAIRS * BLOCK_TOKENS].reshape(BLOCK_PAIRS, BLOCK_TOKENS, HQ)
    later_half = rows_all[BLOCK_PAIRS * BLOCK_TOKENS:].reshape(BLOCK_PAIRS, BLOCK_TOKENS, HQ)[::-1]
    return jnp.stack([earlier_half, later_half], axis=1).astype(jnp.float32)


def shard_levels(key, extent, cuts, least, high):
    gain = 1.0
    for position, shards_of in cuts:
        draws = jax.random.uniform(jax.random.fold_in(jax.random.fold_in(key, 6), position), (shards_of,), jnp.float32, least / len(cuts), high / len(cuts))
        gain = gain * jnp.repeat(jnp.exp(draws), extent[position] // shards_of).reshape((-1,) + (1,) * (len(extent) - 1 - position))
    return gain


def gaussian(key, extent, deviation, bound, cuts=(), held_as=jnp.bfloat16):
    values = jax.random.normal(key, extent, jnp.float32) * deviation
    if len(cuts) > 0:
        values = shard_levels(key, extent, cuts, -0.22, 0.18) * values
    return jnp.clip(values, min=-bound, max=bound).astype(held_as)


def setup_inputs(seed: int = 0, part: int = 0) -> dict:
    streams_of = jax.random.split(jax.random.key(seed), 7)
    part_splits = jax.random.split(jax.random.fold_in(streams_of[6], part), 7)
    return {
        "attention_queries": draw_attention_queries(jax.random.fold_in(jax.random.fold_in(streams_of[6], part), 71), part),
        "attention_keys": draw_attention_keys(jax.random.fold_in(jax.random.fold_in(streams_of[6], part), 71), part),
        "attention_values": gaussian(part_splits[2], (BLOCK_PAIRS, 2, BLOCK_TOKENS, KEY_VALUE_HEADS * HEAD_SIZE), 1.0, 6.0, ((0, 8),)),
        "attention_output": gaussian(part_splits[3], (BLOCK_PAIRS, 2, BLOCK_TOKENS, HQ * HEAD_SIZE), 1.0, 6.0, ((0, 8),)),
        "output_gradient": gaussian(part_splits[4], (BLOCK_PAIRS, 2, BLOCK_TOKENS, HQ * HEAD_SIZE), 8.0, 48.0, ((0, 8),)),
        "logsumexp_rows": draw_logsumexp_rows(jax.random.fold_in(jax.random.fold_in(streams_of[6], part), 71), part),
    }


def blocks_to_sequence(blocks):
    earlier_half = blocks[:, 0].reshape(BLOCK_PAIRS * BLOCK_TOKENS, blocks.shape[-1])
    later_half = blocks[::-1, 1].reshape(BLOCK_PAIRS * BLOCK_TOKENS, blocks.shape[-1])
    return jnp.concatenate([earlier_half, later_half], axis=0)


def to_blocks(sequence):
    earlier_half = sequence[: BLOCK_PAIRS * BLOCK_TOKENS].reshape(BLOCK_PAIRS, BLOCK_TOKENS, sequence.shape[-1])
    later_half = sequence[BLOCK_PAIRS * BLOCK_TOKENS:].reshape(BLOCK_PAIRS, BLOCK_TOKENS, sequence.shape[-1])[::-1]
    return jnp.stack([earlier_half, later_half], axis=1)


def split_low(values):
    high_part = values.astype(jnp.bfloat16)
    back_value = lax.optimization_barrier(high_part).astype(jnp.float32)
    rest_part = (values - back_value).astype(jnp.bfloat16)
    return high_part.astype(jnp.float32), rest_part.astype(jnp.float32)


def reference(attention_queries, attention_keys, attention_values, attention_output, output_gradient, logsumexp_rows):
    scaling = HEAD_SIZE ** -0.5
    sequence_length = 2 * BLOCK_PAIRS * BLOCK_TOKENS
    span_rows = 2 * BLOCK_TOKENS
    query_values_list = blocks_to_sequence(attention_queries).reshape(sequence_length, KEY_VALUE_HEADS, QUERY_PER_KV, HEAD_SIZE)
    gradient_sequence = blocks_to_sequence(output_gradient).reshape(sequence_length, KEY_VALUE_HEADS, QUERY_PER_KV, HEAD_SIZE)
    output_sequence = blocks_to_sequence(attention_output).reshape(sequence_length, KEY_VALUE_HEADS, QUERY_PER_KV, HEAD_SIZE)
    logsum_sequence = blocks_to_sequence(logsumexp_rows).reshape(sequence_length, KEY_VALUE_HEADS, QUERY_PER_KV)
    key_as_float = blocks_to_sequence(attention_keys).reshape(sequence_length, KEY_VALUE_HEADS, HEAD_SIZE).astype(jnp.float32)
    value_as_float = blocks_to_sequence(attention_values).reshape(sequence_length, KEY_VALUE_HEADS, HEAD_SIZE).astype(jnp.float32)
    key_pos = jnp.arange(sequence_length, dtype=jnp.int32)

    def per_block(carried, block_index):
        grad_keys, grad_values = carried
        first_row = (block_index * span_rows).astype(jnp.int32)
        query_blk = lax.dynamic_slice_in_dim(query_values_list, first_row, span_rows, 0).astype(jnp.float32)
        grad_blk = lax.dynamic_slice_in_dim(gradient_sequence, first_row, span_rows, 0).astype(jnp.float32)
        output_blk = lax.dynamic_slice_in_dim(output_sequence, first_row, span_rows, 0).astype(jnp.float32)
        log_blk = lax.dynamic_slice_in_dim(logsum_sequence, first_row, span_rows, 0).transpose(1, 2, 0)[..., None]
        query_pos = first_row + jnp.arange(span_rows, dtype=jnp.int32)
        allowed = key_pos[None, :] <= query_pos[:, None]
        scores = scaling * jnp.einsum("qhgd,khd->hgqk", query_blk, key_as_float)
        weights = jnp.where(allowed, jnp.exp(scores - log_blk), 0.0)
        weights_high, weights_rest = split_low(weights)
        row_delta = jnp.sum(grad_blk * output_blk, axis=-1)
        weight_grad = jnp.einsum("qhgd,khd->hgqk", grad_blk, value_as_float)
        score_grad = weights * (weight_grad - row_delta.transpose(1, 2, 0)[..., None])
        score_high, score_rest = split_low(score_grad)
        grad_values = grad_values + jnp.einsum("hgqk,qhgd->khd", weights_high, grad_blk) + jnp.einsum("hgqk,qhgd->khd", weights_rest, grad_blk)
        grad_keys = grad_keys + scaling * (jnp.einsum("hgqk,qhgd->khd", score_high, query_blk) + jnp.einsum("hgqk,qhgd->khd", score_rest, query_blk))
        grad_query = scaling * (jnp.einsum("hgqk,khd->qhgd", score_high, key_as_float) + jnp.einsum("hgqk,khd->qhgd", score_rest, key_as_float))
        return (grad_keys, grad_values), grad_query

    zero_key_value = jnp.zeros((sequence_length, KEY_VALUE_HEADS, HEAD_SIZE), jnp.float32)
    final_results, grad_blocks = lax.scan(per_block, (zero_key_value, zero_key_value), jnp.arange(BLOCK_PAIRS, dtype=jnp.int32))
    grad_query = grad_blocks.reshape(sequence_length, HQ * HEAD_SIZE)
    key_gradient = final_results[0].reshape(sequence_length, KEY_VALUE_HEADS * HEAD_SIZE)
    value_gradient = final_results[1].reshape(sequence_length, KEY_VALUE_HEADS * HEAD_SIZE)
    return to_blocks(grad_query), to_blocks(key_gradient), to_blocks(value_gradient)
```

```python
import functools

import jax
import jax.numpy as jnp
from jax import lax
from jax.experimental import pallas as pl
from jax.experimental.pallas import tpu as pltpu
from jax.sharding import PartitionSpec as P

HEAD_SIZE = 128
LOG2E = 1.4426950408889634
MESH = pl.DeviceIdType.MESH
KEYS, VALUES = 0, 1
RIGHT, LEFT = 0, 1


def ring_place(index, size):
    return jnp.where(index % 2 == 0, index // 2, size - 1 - index // 2)


def ring_index(place, size):
    return jnp.where(place < size // 2, 2 * place, 2 * (size - 1 - place) + 1)


def split_parts(values):
    high = values.astype(jnp.bfloat16)
    rest = (values - high.astype(jnp.float32)).astype(jnp.bfloat16)
    return jnp.concatenate([high, rest], axis=0)


def dot_rows(a, b):
    return lax.dot_general(a, b, (((1,), (1,)), ((), ())), preferred_element_type=jnp.float32)


def dot(a, b):
    return jnp.dot(a, b, preferred_element_type=jnp.float32)


def kernel(
    n,
    q_ref,
    k_ref,
    v_ref,
    o_ref,
    g_ref,
    lse_ref,
    gq_ref,
    gk_ref,
    gv_ref,
    qs,
    gs,
    delta,
    dqt,
    kv,
    part,
    landed,
    ag_send,
    ag_recv,
    rs_send,
    rs_recv,
):
    half = n // 2
    rows = k_ref.shape[2]
    kv_heads = k_ref.shape[3] // HEAD_SIZE
    group = q_ref.shape[3] // k_ref.shape[3]
    wide = group * rows
    scaling = HEAD_SIZE ** (-0.5)
    me = lax.axis_index("seq")
    place = ring_place(me, n)
    right = ring_index(lax.rem(place + 1, n), n)
    left = ring_index(lax.rem(place + n - 1, n), n)
    target = (right, left)

    barrier = pltpu.get_barrier_semaphore()
    for neighbour in (left, right):
        pl.semaphore_signal(barrier, inc=1, device_id={"seq": neighbour}, device_id_type=MESH)
    pl.semaphore_wait(barrier, 2)

    def gather_copy(way, what, distance, own):
        arrives = n - distance if way == RIGHT else distance
        held = lax.rem(n + 1 - distance, n) if way == RIGHT else distance - 1
        source = (k_ref, v_ref)[what].at[0] if own else kv.at[held, what]
        return pltpu.make_async_remote_copy(
            src_ref=source,
            dst_ref=kv.at[arrives, what],
            send_sem=ag_send.at[way, distance - 1, what],
            recv_sem=ag_recv.at[way, distance - 1, what],
            device_id={"seq": target[way]},
            device_id_type=MESH,
        )

    def sum_copy(what, step, block):
        slot = n - 1 - step if what == KEYS else 1 + step
        return pltpu.make_async_remote_copy(
            src_ref=part.at[what, slot, block],
            dst_ref=landed.at[what, step, block],
            send_sem=rs_send.at[what, step, block],
            recv_sem=rs_recv.at[what, step, block],
            device_id={"seq": target[what]},
            device_id_type=MESH,
        )

    for what in (KEYS, VALUES):
        for way in (RIGHT, LEFT):
            if half > 1 or what == way:
                gather_copy(way, what, 1, True).start()

    def prepare(g, _):
        for a in range(2):
            products = []
            for j in range(group):
                columns = pl.ds(pl.multiple_of((g * group + j) * HEAD_SIZE, HEAD_SIZE), HEAD_SIZE)
                grad = g_ref[0, a, :, columns]
                qs[g, a, pl.ds(j * rows, rows), :] = q_ref[0, a, :, columns]
                gs[g, a, pl.ds(j * rows, rows), :] = grad
                products.append(grad.astype(jnp.float32) * o_ref[0, a, :, columns].astype(jnp.float32))
            turned = jnp.transpose(jnp.concatenate(products, axis=0))
            delta[g, a] = jnp.sum(turned, axis=0, keepdims=True)
            dqt[g, a] = jnp.zeros((HEAD_SIZE, wide), jnp.float32)
        return 0

    lax.fori_loop(0, kv_heads, prepare, 0)

    def unit(key_tile, value_tile, g, a, masked):
        queries, grads = qs[g, a], gs[g, a]
        scores = dot_rows(key_tile, queries)
        weights = jnp.exp2(scores * (scaling * LOG2E) - lse_ref[g, a])
        if masked:
            key_row = lax.broadcasted_iota(jnp.int32, (rows, wide), 0)
            query_row = lax.broadcasted_iota(jnp.int32, (rows, wide), 1) % rows
            weights = jnp.where(key_row <= query_row, weights, 0.0)
        value_part = dot(split_parts(weights), grads)
        score_grad = weights * (dot_rows(value_tile, grads) - delta[g, a])
        split = split_parts(score_grad)
        key_part = dot(split, queries)
        keys_turned = jnp.transpose(jnp.concatenate([key_tile, key_tile], axis=0))
        query_part = dot(keys_turned, split)
        return key_part[:rows] + key_part[rows:], value_part[:rows] + value_part[rows:], query_part

    def columns_of(g):
        return pl.ds(pl.multiple_of(g * HEAD_SIZE, HEAD_SIZE), HEAD_SIZE)

    def shard(slot):
        later = ring_index(lax.rem(place + slot, n), n) > me
        pick = jnp.where(later, 1, 0)

        def head(g, _):
            cols = columns_of(g)
            early = unit(kv[slot, KEYS, 0, :, cols], kv[slot, VALUES, 0, :, cols], g, 1, False)
            other = unit(kv[slot, KEYS, pick, :, cols], kv[slot, VALUES, pick, :, cols], g, pick, False)
            for what in (KEYS, VALUES):
                part[what, slot, 0, :, cols] = early[what] + jnp.where(later, 0.0, other[what])
                part[what, slot, 1, :, cols] = jnp.where(later, other[what], 0.0)
            dqt[g, 1] += early[2]
            dqt[g, pick] += other[2]
            return 0

        lax.fori_loop(0, kv_heads, head, 0)


    def own_shard():
        def head(g, _):
            cols = columns_of(g)
            tiles = [(k_ref[0, b, :, cols], v_ref[0, b, :, cols]) for b in range(2)]
            first = unit(*tiles[0], g, 0, True)
            across = unit(*tiles[0], g, 1, False)
            last = unit(*tiles[1], g, 1, True)
            for what in (KEYS, VALUES):
                part[what, 0, 0, :, cols] = first[what] + across[what]
                part[what, 0, 1, :, cols] = last[what]
            dqt[g, 0] += first[2]
            dqt[g, 1] += across[2] + last[2]
            return 0

        lax.fori_loop(0, kv_heads, head, 0)

    def receive(distance):
        gather_copy(RIGHT, KEYS, distance, False).wait_recv()
        gather_copy(LEFT, VALUES, distance, False).wait_recv()
        gather_copy(RIGHT, VALUES, distance, False).wait_recv()
        gather_copy(LEFT, KEYS, distance, False).wait_recv()

    def send_sums(step, first):
        for block in range(2):
            for what in (KEYS, VALUES):
                if not first:
                    slot = n - 1 - step if what == KEYS else 1 + step
                    sum_copy(what, step - 1, block).wait_recv()
                    part[what, slot, block] += landed[what, step - 1, block]
                sum_copy(what, step, block).start()

    def near(step, first):
        receive(step + 1)

        gather_copy(RIGHT, KEYS, step + 2, False).start()
        gather_copy(LEFT, VALUES, step + 2, False).start()

        @pl.when(step + 2 < half)
        def _():
            gather_copy(RIGHT, VALUES, step + 2, False).start()
            gather_copy(LEFT, KEYS, step + 2, False).start()

        def side(which, _):
            shard(jnp.where(which == 0, n - 1 - step, 1 + step))
            return 0

        lax.fori_loop(0, 2, side, 0)
        send_sums(step, first)

    if half > 1:
        near(0, True)

        def middle(step, _):
            near(step, False)
            return 0

        lax.fori_loop(1, half - 1, middle, 0)

    gather_copy(RIGHT, KEYS, half, False).wait_recv()
    gather_copy(LEFT, VALUES, half, False).wait_recv()
    shard(half)
    send_sums(half - 1, half == 1)

    own_shard()
    for a in range(2):
        def write(g, _):
            turned = jnp.transpose(dqt[g, a]) * scaling
            for j in range(group):
                columns = pl.ds(pl.multiple_of((g * group + j) * HEAD_SIZE, HEAD_SIZE), HEAD_SIZE)
                gq_ref[0, a, :, columns] = turned[j * rows : (j + 1) * rows]
            return 0

        lax.fori_loop(0, kv_heads, write, 0)

    def far(step, _):
        send_sums(step, False)
        return 0

    lax.fori_loop(half, n - 1, far, 0)
    for block in range(2):
        for what in (KEYS, VALUES):
            sum_copy(what, n - 2, block).wait_recv()
            total = part[what, 0, block] + landed[what, n - 2, block]
            if what == KEYS:
                gk_ref[0, block] = total * scaling
            else:
                gv_ref[0, block] = total

    def sent(step, _):
        for block in range(2):
            for what in (KEYS, VALUES):
                sum_copy(what, step, block).wait_send()
        return 0

    lax.fori_loop(0, n - 1, sent, 0)

    def passed(distance, _):
        gather_copy(RIGHT, KEYS, distance, False).wait_send()
        gather_copy(LEFT, VALUES, distance, False).wait_send()
        gather_copy(RIGHT, VALUES, distance, False).wait_send()
        gather_copy(LEFT, KEYS, distance, False).wait_send()
        return 0

    lax.fori_loop(1, half, passed, 0)
    gather_copy(RIGHT, KEYS, half, False).wait_send()
    gather_copy(LEFT, VALUES, half, False).wait_send()


def body(queries, keys, values, output, gradient, logsumexp):
    n = lax.axis_size("seq")
    rows = keys.shape[2]
    kv_heads = keys.shape[3] // HEAD_SIZE
    group = queries.shape[3] // keys.shape[3]
    wide = group * rows
    lse = logsumexp[0].reshape(2, rows, kv_heads, group).transpose(2, 0, 3, 1)
    lse = (lse * LOG2E).reshape(kv_heads, 2, 1, wide)
    vmem = pl.BlockSpec(memory_space=pltpu.VMEM)
    pair = (2, rows, keys.shape[3])
    return pl.pallas_call(
        functools.partial(kernel, n),
        out_shape=(
            jax.ShapeDtypeStruct(queries.shape, jnp.float32),
            jax.ShapeDtypeStruct(keys.shape, jnp.float32),
            jax.ShapeDtypeStruct(values.shape, jnp.float32),
        ),
        in_specs=[vmem] * 6,
        out_specs=(vmem, vmem, vmem),
        scratch_shapes=[
            pltpu.VMEM((kv_heads, 2, wide, HEAD_SIZE), jnp.bfloat16),
            pltpu.VMEM((kv_heads, 2, wide, HEAD_SIZE), jnp.bfloat16),
            pltpu.VMEM((kv_heads, 2, 1, wide), jnp.float32),
            pltpu.VMEM((kv_heads, 2, HEAD_SIZE, wide), jnp.float32),
            pltpu.VMEM((n, 2) + pair, jnp.bfloat16),
            pltpu.VMEM((2, n) + pair, jnp.float32),
            pltpu.VMEM((2, n - 1) + pair, jnp.float32),
            pltpu.SemaphoreType.DMA((2, n // 2, 2)),
            pltpu.SemaphoreType.DMA((2, n // 2, 2)),
            pltpu.SemaphoreType.DMA((2, n - 1, 2)),
            pltpu.SemaphoreType.DMA((2, n - 1, 2)),
        ],
        compiler_params=pltpu.CompilerParams(
            collective_id=0, has_side_effects=True, vmem_limit_bytes=64_000_000
        ),
    )(queries, keys, values, output, gradient, lse)


def solution(mesh):
    spec = P("seq", None, "dp", None)
    return jax.shard_map(
        body, mesh=mesh, in_specs=(spec,) * 6, out_specs=(spec,) * 3, check_vma=False
    )
```

```python
import functools

import jax
import jax.numpy as jnp
from jax import lax
from jax.experimental import pallas as pl
from jax.experimental.pallas import tpu as pltpu
from jax.sharding import PartitionSpec as P

HEAD_SIZE = 128
LOG2E = 1.4426950408889634
MESH = pl.DeviceIdType.MESH
KEYS, VALUES = 0, 1
RIGHT, LEFT = 0, 1
ORDER = ((RIGHT, KEYS), (LEFT, VALUES), (RIGHT, VALUES), (LEFT, KEYS))


def ring_place(index, size):
    return jnp.where(index % 2 == 0, index // 2, size - 1 - index // 2)


def ring_index(place, size):
    return jnp.where(place < size // 2, 2 * place, 2 * (size - 1 - place) + 1)


def split_parts(values):
    high = values.astype(jnp.bfloat16)
    rest = (values - high.astype(jnp.float32)).astype(jnp.bfloat16)
    return jnp.concatenate([high, rest], axis=0)


def dot_rows(a, b):
    return lax.dot_general(a, b, (((1,), (1,)), ((), ())), preferred_element_type=jnp.float32)


def dot(a, b):
    return jnp.dot(a, b, preferred_element_type=jnp.float32)


def kernel(
    n,
    q_ref,
    k_ref,
    v_ref,
    o_ref,
    g_ref,
    lse_ref,
    gq_ref,
    gk_ref,
    gv_ref,
    qs,
    gs,
    delta,
    lse,
    dqt,
    kv,
    part,
    landed,
    ag_send,
    ag_recv,
    rs_send,
    rs_recv,
):
    half = n // 2
    rows = k_ref.shape[2]
    kv_heads = k_ref.shape[3] // HEAD_SIZE
    group = q_ref.shape[3] // k_ref.shape[3]
    wide = group * rows
    scaling = HEAD_SIZE ** (-0.5)
    me = lax.axis_index("seq")
    place = ring_place(me, n)
    right = ring_index(lax.rem(place + 1, n), n)
    left = ring_index(lax.rem(place + n - 1, n), n)
    target = (right, left)

    barrier = pltpu.get_barrier_semaphore()
    for neighbour in (left, right):
        pl.semaphore_signal(barrier, inc=1, device_id={"seq": neighbour}, device_id_type=MESH)
    pl.semaphore_wait(barrier, 2)

    def gather_copy(way, what, distance, own):
        arrives = n - distance if way == RIGHT else distance
        held = lax.rem(n + 1 - distance, n) if way == RIGHT else distance - 1
        source = (k_ref, v_ref)[what].at[0] if own else kv.at[held, what]
        return pltpu.make_async_remote_copy(
            src_ref=source,
            dst_ref=kv.at[arrives, what],
            send_sem=ag_send.at[way, distance - 1, what],
            recv_sem=ag_recv.at[way, distance - 1, what],
            device_id={"seq": target[way]},
            device_id_type=MESH,
        )

    def sum_copy(what, step, block):
        slot = n - 1 - step if what == KEYS else 1 + step
        return pltpu.make_async_remote_copy(
            src_ref=part.at[what, slot, block],
            dst_ref=landed.at[what, step, block],
            send_sem=rs_send.at[what, step, block],
            recv_sem=rs_recv.at[what, step, block],
            device_id={"seq": target[what]},
            device_id_type=MESH,
        )

    for way, what in ORDER:
        if half > 1 or what == way:
            gather_copy(way, what, 1, True).start()

    def pass_on(step):
        for way, what in ORDER:
            gather_copy(way, what, step + 1, False).wait_recv()
            onward = gather_copy(way, what, step + 2, False)
            if what == way:
                onward.start()
            else:
                pl.when(step + 2 < half)(onward.start)

    def prepare(g, _):
        for a in range(2):
            products = []
            logs = lse_ref[0, a, pl.ds(pl.multiple_of(g * group, group), group), :] * LOG2E
            lse[g, a] = jnp.concatenate([logs[j : j + 1] for j in range(group)], axis=1)
            for j in range(group):
                columns = pl.ds(pl.multiple_of((g * group + j) * HEAD_SIZE, HEAD_SIZE), HEAD_SIZE)
                grad = g_ref[0, a, :, columns]
                qs[g, a, pl.ds(j * rows, rows), :] = q_ref[0, a, :, columns]
                gs[g, a, pl.ds(j * rows, rows), :] = grad
                products.append(grad.astype(jnp.float32) * o_ref[0, a, :, columns].astype(jnp.float32))
            turned = jnp.transpose(jnp.concatenate(products, axis=0))
            delta[g, a] = jnp.sum(turned, axis=0, keepdims=True)
            dqt[g, a] = jnp.zeros((HEAD_SIZE, wide), jnp.float32)
        return 0

    lax.fori_loop(0, kv_heads // 2, prepare, 0)
    if half > 1:
        pass_on(0)
    lax.fori_loop(kv_heads // 2, kv_heads, prepare, 0)

    def unit(key_tile, value_tile, g, a, masked):
        queries, grads = qs[g, a], gs[g, a]
        scores = dot_rows(key_tile, queries)
        weights = jnp.exp2(scores * (scaling * LOG2E) - lse[g, a])
        if masked:
            key_row = lax.broadcasted_iota(jnp.int32, (rows, wide), 0)
            query_row = lax.broadcasted_iota(jnp.int32, (rows, wide), 1) % rows
            weights = jnp.where(key_row <= query_row, weights, 0.0)
        value_part = dot(split_parts(weights), grads)
        score_grad = weights * (dot_rows(value_tile, grads) - delta[g, a])
        split = split_parts(score_grad)
        key_part = dot(split, queries)
        keys_turned = jnp.transpose(jnp.concatenate([key_tile, key_tile], axis=0))
        query_part = dot(keys_turned, split)
        return key_part[:rows] + key_part[rows:], value_part[:rows] + value_part[rows:], query_part

    def columns_of(g):
        return pl.ds(pl.multiple_of(g * HEAD_SIZE, HEAD_SIZE), HEAD_SIZE)

    def shard(slot):
        later = ring_index(lax.rem(place + slot, n), n) > me
        pick = jnp.where(later, 1, 0)

        def head(g, _):
            cols = columns_of(g)
            early = unit(kv[slot, KEYS, 0, :, cols], kv[slot, VALUES, 0, :, cols], g, 1, False)
            other = unit(kv[slot, KEYS, pick, :, cols], kv[slot, VALUES, pick, :, cols], g, pick, False)
            for what in (KEYS, VALUES):
                part[what, slot, 0, :, cols] = early[what] + jnp.where(later, 0.0, other[what])
                part[what, slot, 1, :, cols] = jnp.where(later, other[what], 0.0)
            dqt[g, 1] += early[2]
            dqt[g, pick] += other[2]
            return 0

        lax.fori_loop(0, kv_heads, head, 0)


    def own_shard():
        def head(g, _):
            cols = columns_of(g)
            tiles = [(k_ref[0, b, :, cols], v_ref[0, b, :, cols]) for b in range(2)]
            first = unit(*tiles[0], g, 0, True)
            across = unit(*tiles[0], g, 1, False)
            last = unit(*tiles[1], g, 1, True)
            for what in (KEYS, VALUES):
                part[what, 0, 0, :, cols] = first[what] + across[what]
                part[what, 0, 1, :, cols] = last[what]
            dqt[g, 0] += first[2]
            dqt[g, 1] += across[2] + last[2]
            return 0

        lax.fori_loop(0, kv_heads, head, 0)

    def send_sum(what, step, block, first):
        if not first:
            slot = n - 1 - step if what == KEYS else 1 + step
            sum_copy(what, step - 1, block).wait_recv()
            part[what, slot, block] += landed[what, step - 1, block]
        sum_copy(what, step, block).start()

    def send_sums(step, first):
        for block in range(2):
            for what in (KEYS, VALUES):
                send_sum(what, step, block, first)

    def near(step, first):
        for what in (KEYS, VALUES):
            shard(n - 1 - step if what == KEYS else 1 + step)
            for block in range(2):
                send_sum(what, step, block, first)

    if half > 1:
        near(0, True)

        def middle(step, _):
            pass_on(step)
            near(step, False)
            return 0

        lax.fori_loop(1, half - 1, middle, 0)

    gather_copy(RIGHT, KEYS, half, False).wait_recv()
    gather_copy(LEFT, VALUES, half, False).wait_recv()
    shard(half)
    send_sums(half - 1, half == 1)

    own_shard()
    for a in range(2):
        if half + a < n - 1:
            send_sums(half + a, False)

        def write(g, _):
            turned = jnp.transpose(dqt[g, a]) * scaling
            for j in range(group):
                columns = pl.ds(pl.multiple_of((g * group + j) * HEAD_SIZE, HEAD_SIZE), HEAD_SIZE)
                gq_ref[0, a, :, columns] = turned[j * rows : (j + 1) * rows]
            return 0

        lax.fori_loop(0, kv_heads, write, 0)

    def far(step, _):
        send_sums(step, False)
        return 0

    lax.fori_loop(half + 2, n - 1, far, 0)
    for block in range(2):
        for what in (KEYS, VALUES):
            sum_copy(what, n - 2, block).wait_recv()
            total = part[what, 0, block] + landed[what, n - 2, block]
            if what == KEYS:
                gk_ref[0, block] = total * scaling
            else:
                gv_ref[0, block] = total

    def sent(step, _):
        for block in range(2):
            for what in (KEYS, VALUES):
                sum_copy(what, step, block).wait_send()
        return 0

    lax.fori_loop(0, n - 1, sent, 0)

    def passed(distance, _):
        gather_copy(RIGHT, KEYS, distance, False).wait_send()
        gather_copy(LEFT, VALUES, distance, False).wait_send()
        gather_copy(RIGHT, VALUES, distance, False).wait_send()
        gather_copy(LEFT, KEYS, distance, False).wait_send()
        return 0

    lax.fori_loop(1, half, passed, 0)
    gather_copy(RIGHT, KEYS, half, False).wait_send()
    gather_copy(LEFT, VALUES, half, False).wait_send()


def body(queries, keys, values, output, gradient, logsumexp):
    n = lax.axis_size("seq")
    rows = keys.shape[2]
    kv_heads = keys.shape[3] // HEAD_SIZE
    group = queries.shape[3] // keys.shape[3]
    wide = group * rows
    lse = logsumexp.transpose(0, 1, 3, 2)
    shard_bytes = 2 * 2 * rows * keys.shape[3]
    limit = (20 << 20) + n * shard_bytes * 10
    vmem = pl.BlockSpec(memory_space=pltpu.VMEM)
    pair = (2, rows, keys.shape[3])
    return pl.pallas_call(
        functools.partial(kernel, n),
        out_shape=(
            jax.ShapeDtypeStruct(queries.shape, jnp.float32),
            jax.ShapeDtypeStruct(keys.shape, jnp.float32),
            jax.ShapeDtypeStruct(values.shape, jnp.float32),
        ),
        in_specs=[vmem] * 6,
        out_specs=(vmem, vmem, vmem),
        scratch_shapes=[
            pltpu.VMEM((kv_heads, 2, wide, HEAD_SIZE), jnp.bfloat16),
            pltpu.VMEM((kv_heads, 2, wide, HEAD_SIZE), jnp.bfloat16),
            pltpu.VMEM((kv_heads, 2, 1, wide), jnp.float32),
            pltpu.VMEM((kv_heads, 2, 1, wide), jnp.float32),
            pltpu.VMEM((kv_heads, 2, HEAD_SIZE, wide), jnp.float32),
            pltpu.VMEM((n, 2) + pair, jnp.bfloat16),
            pltpu.VMEM((2, n) + pair, jnp.float32),
            pltpu.VMEM((2, n - 1) + pair, jnp.float32),
            pltpu.SemaphoreType.DMA((2, n // 2, 2)),
            pltpu.SemaphoreType.DMA((2, n // 2, 2)),
            pltpu.SemaphoreType.DMA((2, n - 1, 2)),
            pltpu.SemaphoreType.DMA((2, n - 1, 2)),
        ],
        compiler_params=pltpu.CompilerParams(
            collective_id=0, has_side_effects=True, vmem_limit_bytes=limit
        ),
    )(queries, keys, values, output, gradient, lse)


def solution(mesh):
    spec = P("seq", None, "dp", None)
    return jax.shard_map(
        body, mesh=mesh, in_specs=(spec,) * 6, out_specs=(spec,) * 3, check_vma=False
    )
```
